128 devices in a mesh: pa: 128 (over x, z, y, core).
Axes of the slice: x: 4, y: 4, z: 4, core: 2. Of those that a mesh axis runs over, the one named last changes fastest.
Arguments:
- image_real: float32 [8, 4096, 4096], P(None, 'pa'), may hold values from -6 to 6
- image_imag: float32 [8, 4096, 4096], P(None, 'pa'), may hold values from -6 to 6
Outputs:
- spectrum_real: float32 [8, 4096, 4096], P(None, 'pa')
- spectrum_imag: float32 [8, 4096, 4096], P(None, 'pa')
The draws below stay inside these ranges and needn't reach their ends.
All inputs are finite; a program needn't handle non-finite values.
Results may differ from the reference program's by a relative error of at most 0.0003.
Values sent between devices are 32-bit elements.
No kernel may reach another device: no remote copies, remote signals or barrier semaphores. Data moves between devices by JAX's collectives and lax.ppermute only.
A program may use at most 256 MiB of HBM per device.

```python
import math
import jax
import jax.numpy as jnp
from jax import lax

N = 4096
FRAMES = 8


def levels(rng, dims, cuts, least, high):
    def one(position, shards_of):
        draws = jax.random.uniform(jax.random.fold_in(jax.random.fold_in(rng, 6), position), (shards_of,), jnp.float32, least / len(cuts), high / len(cuts))
        return jnp.repeat(jnp.exp(draws), dims[position] // shards_of).reshape((-1,) + (1,) * (len(dims) - position - 1))

    factor_of = one(*cuts[0])
    for cut in cuts[1:]:
        factor_of = factor_of * one(*cut)
    return factor_of


def gaussian(key, shape, width, most, shards=(), held_as=jnp.bfloat16):
    gain = levels(key, shape, shards, -0.22, 0.18) if shards else 1.0
    result = jax.random.normal(key, shape, jnp.float32) * width * gain
    return jnp.minimum(jnp.maximum(result, -most), most).astype(held_as)


def setup_inputs(seed: int = 0) -> dict:
    key_of = jax.random.split(jax.random.key(seed), 3)
    image_real = gaussian(key_of[0], (FRAMES, N, N), 1.0, 6.0, ((1, 128),), jnp.float32)
    image_imag = gaussian(key_of[1], (FRAMES, N, N), 1.0, 6.0, ((1, 128),), jnp.float32)
    return {"image_real": image_real, "image_imag": image_imag}


canceller_gain = 1.0 / math.sqrt(6.0)

def hamming(offset, sample_count, length):
    sample_index = (offset + jnp.arange(sample_count, dtype=jnp.int32)).astype(jnp.float32)
    return 0.54 - 0.46 * jnp.cos(sample_index * (2.0 * math.pi / length))

def cancel_along(extended, time_axis):
    extent = extended.shape[time_axis]
    newest = lax.slice_in_dim(extended, 2, extent, axis=time_axis)
    middle = lax.slice_in_dim(extended, 1, extent - 1, axis=time_axis)
    oldest = lax.slice_in_dim(extended, 0, extent - 2, axis=time_axis)
    return (newest - 2.0 * middle + oldest) * canceller_gain

def reference(image_real, image_imag):
    window = hamming(0, N, N)

    def one_frame(pieces):
        real_part, imag_part = pieces
        padded = jnp.pad(jnp.stack([real_part, imag_part]), ((0, 0), (2, 0), (0, 0)))
        weighted = cancel_along(padded, 1) * window[:, None] * window[None, :]
        spectrum = jnp.fft.fft2(weighted[0] + 1j * weighted[1], norm='ortho')
        return (jnp.transpose(spectrum.real), jnp.transpose(spectrum.imag))
    spectrum_real, spectrum_imag = lax.map(one_frame, (image_real, image_imag))
    return (spectrum_real, spectrum_imag)
```

```python
import functools
import math

import jax
import jax.numpy as jnp
import numpy as np
from jax import lax
from jax.experimental import pallas as pl
from jax.experimental.pallas import tpu as pltpu
from jax.sharding import PartitionSpec as P

N = 4096
SHORT = 32
LONG = 128
LANES = 128
SUB = 8
ROOT_HALF = math.sqrt(0.5)


def hamming(index):
    return 0.54 - 0.46 * jnp.cos(index.astype(jnp.float32) * (2.0 * math.pi / N))


def twiddles():
    angle = -2.0 * np.pi * (np.arange(SHORT)[:, None] * np.arange(LONG)[None, :]) / N
    wide = np.repeat(np.stack([np.cos(angle), np.sin(angle)]), SUB, axis=1)
    return wide.astype(np.float32)


def long_matrix():
    angle = -2.0 * np.pi * ((np.arange(LONG)[:, None] * np.arange(LONG)[None, :]) % LONG) / LONG
    real, imag = np.cos(angle), np.sin(angle)
    whole = np.block([[real, imag], [-imag, real]]).astype(np.float32)
    high = whole.astype(jnp.bfloat16)
    low = (whole - high.astype(np.float32)).astype(jnp.bfloat16)
    return high, low


def add(a, b):
    return a[0] + b[0], a[1] + b[1]


def sub(a, b):
    return a[0] - b[0], a[1] - b[1]


def minus_i(a):
    return a[1], -a[0]


def times(a, angle):
    c, s = math.cos(angle), math.sin(angle)
    return a[0] * c - a[1] * s, a[0] * s + a[1] * c


def rotate(a, power):
    power %= 32
    if power == 0:
        return a
    if power == 8:
        return minus_i(a)
    if power == 4:
        return (a[0] + a[1]) * ROOT_HALF, (a[1] - a[0]) * ROOT_HALF
    if power == 12:
        return (a[1] - a[0]) * ROOT_HALF, (a[0] + a[1]) * -ROOT_HALF
    return times(a, -2.0 * math.pi * power / 32)


def dft4(x):
    s, d = add(x[0], x[2]), sub(x[0], x[2])
    t, e = add(x[1], x[3]), sub(x[1], x[3])
    e = minus_i(e)
    return [add(s, t), add(d, e), sub(s, t), sub(d, e)]


def dft8(x):
    even, odd = dft4(x[0::2]), dft4(x[1::2])
    odd = [rotate(v, 4 * k) for k, v in enumerate(odd)]
    return [add(a, b) for a, b in zip(even, odd)] + [sub(a, b) for a, b in zip(even, odd)]


def dft32(load, store):
    parts = []
    for r in range(4):
        part = dft8([load(4 * i + r) for i in range(8)])
        parts.append([rotate(v, r * k) for k, v in enumerate(part)])
    for k in range(8):
        for q, value in enumerate(dft4([parts[r][k] for r in range(4)])):
            store(k + 8 * q, value)


def split(value):
    high = value.astype(jnp.bfloat16)
    return high, (value - high.astype(jnp.float32)).astype(jnp.bfloat16)


def matmul3(high_ref, low_ref, mat_ref, out_ref):
    dot = functools.partial(jnp.dot, preferred_element_type=jnp.float32)
    high, low = high_ref[...], low_ref[...]
    out_ref[...] = dot(high, mat_ref[0]) + dot(low, mat_ref[0]) + dot(high, mat_ref[1])


def tile(i):
    return pl.ds(i * LANES, LANES)


def short_stage(planes, row0, col_ref, tw_ref, z_ref, z_row):
    def load(a):
        w = col_ref[:, tile(a)]
        return tuple(p[pl.ds(row0, SUB), tile(a)] * w for p in planes)

    def store(k, value):
        real, imag = value
        if k:
            c, s = tw_ref[0, pl.ds(k * SUB, SUB), :], tw_ref[1, pl.ds(k * SUB, SUB), :]
            real, imag = real * c - imag * s, real * s + imag * c
        z_ref[0, pl.ds(z_row + k * SUB, SUB), :] = real
        z_ref[1, pl.ds(z_row + k * SUB, SUB), :] = imag

    dft32(load, store)


def pre_kernel(row_ref, real_ref, imag_ref, hr_ref, hi_ref, col_ref, tw_ref, mat_ref, out_ref, z_ref, edge_ref, high_ref, low_ref, y_ref):
    frame = pl.program_id(0)

    @pl.when(frame % 4 == 0)
    def _():
        short_stage((hr_ref, hi_ref), pl.multiple_of(frame // 4 * SUB, SUB), col_ref, tw_ref, edge_ref, 0)

    for block in range(4):
        short_stage((real_ref.at[0], imag_ref.at[0]), block * SUB, col_ref, tw_ref, z_ref, block * SHORT * SUB)

    for plane in range(2):

        def rows(js):
            return z_ref[plane, pl.ds(js, LANES, stride=SUB), :]

        def rows_before(js):
            edge = edge_ref[plane, pl.ds(frame % 4 * 2 + js - 6, SHORT, stride=SUB), :]
            return jnp.concatenate([edge, z_ref[plane, pl.ds(js, 3 * SHORT, stride=SUB), :]], axis=0)

        before = rows_before(7)
        slope = before - rows_before(6)
        for js in range(SUB):
            now = rows(js)
            new_slope = now - before
            value = new_slope - slope
            before, slope = now, new_slope
            for b in range(4):
                high, low = split(value[b * SHORT : (b + 1) * SHORT] * row_ref[b * SUB + js])
                high_ref[pl.ds(js * LANES + b * SHORT, SHORT), tile(plane)] = high
                low_ref[pl.ds(js * LANES + b * SHORT, SHORT), tile(plane)] = low

    matmul3(high_ref, low_ref, mat_ref, y_ref)

    flat = out_ref.reshape(LANES * 16, LANES)
    for js in range(SUB):
        for plane in range(2):
            piece = y_ref[pl.ds(js * LANES, LANES), tile(plane)]
            flat[pl.ds(js * 2 + plane, LANES, stride=16), :] = piece.T


def post_kernel(in_ref, tw_ref, mat_ref, real_ref, imag_ref, high_ref, low_ref, y_ref):
    flat = in_ref.reshape(LANES * 16, LANES)
    for js in range(SUB):
        for plane in range(2):
            piece = flat[pl.ds(js * 2 + plane, LANES, stride=16), :].T
            high, low = split(piece)
            high_ref[pl.ds(js * LANES, LANES), tile(plane)] = high
            low_ref[pl.ds(js * LANES, LANES), tile(plane)] = low

    matmul3(high_ref, low_ref, mat_ref, y_ref)

    for block in range(4):

        def load(j):
            row = ((j % SUB) * 4 + j // SUB) * SHORT + block * SUB
            real, imag = y_ref[pl.ds(row, SUB), tile(0)], y_ref[pl.ds(row, SUB), tile(1)]
            if j:
                c, s = tw_ref[0, pl.ds(j * SUB, SUB), :], tw_ref[1, pl.ds(j * SUB, SUB), :]
                real, imag = real * c - imag * s, real * s + imag * c
            return real, imag

        def store(k, value):
            real_ref[0, pl.ds(block * SUB, SUB), tile(k)] = value[0]
            imag_ref[0, pl.ds(block * SUB, SUB), tile(k)] = value[1]

        dft32(load, store)


def pre(row, real, imag, halo_real, halo_imag, col, tw, mat):
    frames = real.shape[0]
    f32 = jnp.float32
    frame = pl.BlockSpec((1, SHORT, N), lambda f: (f, 0, 0))
    whole = lambda shape: pl.BlockSpec(shape, lambda f: (0,) * len(shape))
    return pl.pallas_call(
        pre_kernel,
        grid=(frames,),
        in_specs=[
            pl.BlockSpec(memory_space=pltpu.SMEM),
            frame,
            frame,
            whole(halo_real.shape),
            whole(halo_imag.shape),
            whole(col.shape),
            whole(tw.shape),
            whole(mat.shape),
        ],
        out_specs=pl.BlockSpec((LANES, 16, LANES), lambda f: (0, f, 0)),
        out_shape=jax.ShapeDtypeStruct((LANES, frames * 16, LANES), f32),
        scratch_shapes=[
            pltpu.VMEM((2, 4 * SHORT * SUB, LANES), f32),
            pltpu.VMEM((2, SHORT * SUB, LANES), f32),
            pltpu.VMEM((4 * SHORT * SUB, 2 * LANES), jnp.bfloat16),
            pltpu.VMEM((4 * SHORT * SUB, 2 * LANES), jnp.bfloat16),
            pltpu.VMEM((4 * SHORT * SUB, 2 * LANES), f32),
        ],
        name="pre",
    )(row, real, imag, halo_real, halo_imag, col, tw, mat)


def post(blocks, tw, mat):
    frames = blocks.shape[1] // 16
    f32 = jnp.float32
    frame = pl.BlockSpec((1, SHORT, N), lambda f: (f, 0, 0))
    whole = lambda shape: pl.BlockSpec(shape, lambda f: (0,) * len(shape))
    return pl.pallas_call(
        post_kernel,
        grid=(frames,),
        in_specs=[pl.BlockSpec((LANES, 16, LANES), lambda f: (0, f, 0)), whole(tw.shape), whole(mat.shape)],
        out_specs=[frame, frame],
        out_shape=[jax.ShapeDtypeStruct((frames, SHORT, N), f32)] * 2,
        scratch_shapes=[
            pltpu.VMEM((4 * SHORT * SUB, 2 * LANES), jnp.bfloat16),
            pltpu.VMEM((4 * SHORT * SUB, 2 * LANES), jnp.bfloat16),
            pltpu.VMEM((4 * SHORT * SUB, 2 * LANES), f32),
        ],
        name="post",
    )(blocks, tw, mat)


def from_behind(value):
    count = lax.axis_size("pa")
    return lax.ppermute(value, "pa", [(i, i + 1) for i in range(count - 1)])


def on_device(real, imag):
    frames, rows, _ = real.shape
    me = lax.axis_index("pa")
    halo = from_behind(jnp.stack([real[:, rows - 2 :], imag[:, rows - 2 :]]))
    halo = halo.reshape(2, frames * 2, N)
    row = hamming(me * rows + jnp.arange(rows, dtype=jnp.int32)) * (1.0 / (math.sqrt(6.0) * N))
    col = jnp.broadcast_to(hamming(jnp.arange(N, dtype=jnp.int32)), (SUB, N))
    tw = jnp.asarray(twiddles())
    mat = jnp.stack([jnp.asarray(m) for m in long_matrix()])
    sent = pre(row, real, imag, halo[0], halo[1], col, tw, mat)
    got = lax.all_to_all(sent, "pa", split_axis=0, concat_axis=0, tiled=True)
    return tuple(post(got, tw, mat))


def solution(mesh):
    placed = (P(None, "pa", None), P(None, "pa", None))
    return jax.shard_map(on_device, mesh=mesh, in_specs=placed, out_specs=placed, check_vma=False)
```

```python
import functools
import math

import jax
import jax.numpy as jnp
import numpy as np
from jax import lax
from jax.experimental import pallas as pl
from jax.experimental.pallas import tpu as pltpu
from jax.sharding import PartitionSpec as P


N = 4096
FRAMES = 8
SHORT = 32
LONG = 128
LANES = 128
SUB = 8
ROWS = 4 * SHORT * SUB
ROOT_HALF = math.sqrt(0.5)

EDGES = (4, 2, 0, 5, 3, 1)
ORDERS = (
    ((2, 1, 0, 4, 5, 3), (5, 4, 3, 1, 2, 0)),
    ((1, 0, 2, 5, 3, 4), (4, 3, 5, 2, 0, 1)),
    ((0, 2, 1, 3, 4, 5), (3, 5, 4, 0, 1, 2)),
    ((2, 1, 0, 4, 5, 3), (5, 4, 3, 1, 2, 0)),
    ((1, 0, 2, 5, 3, 4), (4, 3, 5, 2, 0, 1)),
    ((0, 2, 1, 3, 4, 5), (3, 5, 4, 0, 1, 2)),
    ((2, 1, 0, 4, 5, 3), (5, 4, 3, 1, 2, 0)),
    ((0, 1, 2, 3, 5, 4), (3, 4, 5, 0, 2, 1)),
)
STEPS = len(EDGES)
SLOTS = 64
GROUPS = ((0, 2), (2, 2), (4, 4))


def recode(chip):
    return chip ^ (chip >> 1 & 21)


def edges_of(frame, core):
    return [EDGES[e] for e in ORDERS[frame][core]]


def edge_pairs(frame, step):
    pairs = []
    for device in range(2 * SLOTS):
        chip, core = divmod(device, 2)
        partner = recode(recode(chip) ^ (1 << edges_of(frame, core)[step]))
        pairs.append((device, partner * 2 + core))
    return pairs


def peer(me, frame, core_bit, steps):
    core = me % 2 ^ core_bit
    masks = [sum(bit << edge for bit, edge in zip(steps, edges_of(frame, c))) for c in range(2)]
    return recode(recode(me // 2) ^ jnp.where(core == 0, *masks)) * 2 + core


def targets(me, frame):
    slot = jnp.arange(2 * SLOTS, dtype=jnp.int32)
    return peer(me, frame, slot >> STEPS, [slot >> (STEPS - 1 - k) & 1 for k in range(STEPS)])


def sources(me, frame):
    slot = jnp.arange(2 * SLOTS, dtype=jnp.int32)
    masks = [sum((slot >> (k + 1) & 1) << edge for k, edge in enumerate(edges_of(frame, c))) for c in range(2)]
    return recode(recode(me // 2) ^ jnp.where(me % 2 == 0, *masks)) * 2 + (me % 2 ^ slot & 1)


def hamming(index):
    return 0.54 - 0.46 * jnp.cos(index.astype(jnp.float32) * (2.0 * math.pi / N))


def column_window():
    window = 0.54 - 0.46 * np.cos(2.0 * np.pi * np.arange(N) / N)
    return window.astype(np.float32)[None]


def twiddles():
    angle = -2.0 * np.pi * (np.arange(SHORT)[:, None] * np.arange(LONG)[None, :]) / N
    wide = np.repeat(np.stack([np.cos(angle), np.sin(angle)]), SUB, axis=1)
    return wide.astype(np.float32)


def long_matrix():
    phase = np.arange(LONG)[:, None] * np.arange(LONG)[None, :] % LONG
    angle = -2.0 * np.pi * phase / LONG
    real, imag = np.cos(angle), np.sin(angle)
    whole = np.block([[real, imag], [-imag, real]]).astype(np.float32)
    high = whole.astype(jnp.bfloat16)
    return np.stack([high, (whole - high.astype(np.float32)).astype(jnp.bfloat16)])


def add(a, b):
    return a[0] + b[0], a[1] + b[1]


def sub(a, b):
    return a[0] - b[0], a[1] - b[1]


def minus_i(a):
    return a[1], -a[0]


def times(a, angle):
    c, s = math.cos(angle), math.sin(angle)
    return a[0] * c - a[1] * s, a[0] * s + a[1] * c


def rotate(a, power):
    power %= 32
    if power == 0:
        return a
    if power == 8:
        return minus_i(a)
    if power == 4:
        return (a[0] + a[1]) * ROOT_HALF, (a[1] - a[0]) * ROOT_HALF
    if power == 12:
        return (a[1] - a[0]) * ROOT_HALF, (a[0] + a[1]) * -ROOT_HALF
    return times(a, -2.0 * math.pi * power / 32)


def dft4(x):
    s, d = add(x[0], x[2]), sub(x[0], x[2])
    t, e = add(x[1], x[3]), sub(x[1], x[3])
    e = minus_i(e)
    return [add(s, t), add(d, e), sub(s, t), sub(d, e)]


def dft8(x):
    even, odd = dft4(x[0::2]), dft4(x[1::2])
    odd = [rotate(v, 4 * k) for k, v in enumerate(odd)]
    return [add(a, b) for a, b in zip(even, odd)] + [sub(a, b) for a, b in zip(even, odd)]


def dft32(load, store):
    parts = []
    for r in range(4):
        part = dft8([load(4 * i + r) for i in range(8)])
        parts.append([rotate(v, r * k) for k, v in enumerate(part)])
    for k in range(8):
        for q, value in enumerate(dft4([parts[r][k] for r in range(4)])):
            store(k + 8 * q, value)


def split(value):
    high = value.astype(jnp.bfloat16)
    return high, (value - high.astype(jnp.float32)).astype(jnp.bfloat16)


def matmul3(high_ref, low_ref, mat_ref, out_ref):
    dot = functools.partial(jnp.dot, preferred_element_type=jnp.float32)
    high, low = high_ref[...], low_ref[...]
    out_ref[...] = dot(high, mat_ref[0]) + dot(low, mat_ref[0]) + dot(high, mat_ref[1])


def tile(i):
    return pl.ds(i * LANES, LANES)


def short_stage(planes, row0, col_ref, tw_ref, z_ref, z_row):
    def load(a):
        w = col_ref[:, tile(a)]
        return tuple(p[pl.ds(row0, SUB), tile(a)] * w for p in planes)

    def store(k, value):
        real, imag = value
        if k:
            c, s = tw_ref[0, pl.ds(k * SUB, SUB), :], tw_ref[1, pl.ds(k * SUB, SUB), :]
            real, imag = real * c - imag * s, real * s + imag * c
        z_ref[0, pl.ds(z_row + k * SUB, SUB), :] = real
        z_ref[1, pl.ds(z_row + k * SUB, SUB), :] = imag

    dft32(load, store)


def matrix_kernel(target_ref, source_ref, base_ref, forward_ref, backward_ref):
    dot = functools.partial(jnp.dot, preferred_element_type=jnp.float32)
    square = (LONG, LONG)
    for frame in range(len(ORDERS)):
        wanted = jnp.broadcast_to(target_ref[pl.ds(frame, 1), :], square)
        pick = (wanted == lax.broadcasted_iota(jnp.int32, square, 0)).astype(jnp.bfloat16)
        wanted = jnp.broadcast_to(source_ref[:, pl.ds(frame, 1)], square)
        place = (wanted == lax.broadcasted_iota(jnp.int32, square, 1)).astype(jnp.bfloat16)
        for part in range(2):
            for half in range(2):
                forward_ref[frame, part, :, tile(half)] = dot(base_ref[part, :, tile(half)], pick).astype(jnp.bfloat16)
                backward_ref[frame, part, tile(half), :] = dot(place, base_ref[part, tile(half), :]).astype(jnp.bfloat16)


def last_kernel(real_ref, imag_ref, out_a_ref, out_b_ref, rows_ref, sem):
    copies = [
        pltpu.make_async_copy(ref.at[:, pl.ds(SHORT - SUB, SUB)], rows_ref.at[plane], sem.at[plane])
        for plane, ref in enumerate((real_ref, imag_ref))
    ]
    for copy in copies:
        copy.start()
    for plane, copy in enumerate(copies):
        copy.wait()
        for frame in range(FRAMES):
            out = (out_a_ref, out_b_ref)[frame // 4]
            out[plane, pl.ds(frame % 4 * 2, 2), :] = rows_ref[plane, frame, pl.ds(SUB - 2, 2), :]


def short_kernel(real_ref, imag_ref, col_ref, tw_ref, z_ref):
    z = z_ref.at[pl.program_id(0)]

    @pl.loop(0, 4)
    def _(block):
        row = pl.multiple_of(block * SUB, SUB)
        short_stage((real_ref.at[0], imag_ref.at[0]), row, col_ref, tw_ref, z, pl.multiple_of(row * SHORT, SUB * SHORT))


def edge_kernel(halo_ref, col_ref, tw_ref, out_ref):
    short_stage((halo_ref.at[0], halo_ref.at[1]), 0, col_ref, tw_ref, out_ref, 0)


def pre_kernel(row_ref, z_ref, edge_ref, mat_ref, keep_ref, send_ref, high_ref, low_ref, y_ref, *, first):
    local = pl.program_id(0)
    frame = first + local
    for plane in range(2):

        def rows(js):
            return z_ref[local, plane, pl.ds(js, LANES, stride=SUB), :]

        def rows_before(js):
            edge = edge_ref[plane, pl.ds(frame % 4 * 2 + js - 6, SHORT, stride=SUB), :]
            return jnp.concatenate([edge, z_ref[local, plane, pl.ds(js, 3 * SHORT, stride=SUB), :]], axis=0)

        before = rows_before(7)
        slope = before - rows_before(6)
        for js in range(SUB):
            now = rows(js)
            new_slope = now - before
            value = new_slope - slope
            before, slope = now, new_slope
            for b in range(4):
                part = value[b * SHORT : (b + 1) * SHORT].reshape(SHORT // SUB, SUB, LANES)
                part = part * row_ref[pl.ds((b * SUB + js) * SUB, SUB), :]
                high, low = split(part.reshape(SHORT, LANES))
                high_ref[pl.ds(js * LANES + b * SHORT, SHORT), tile(plane)] = high
                low_ref[pl.ds(js * LANES + b * SHORT, SHORT), tile(plane)] = low

    matmul3(high_ref, low_ref, mat_ref.at[frame], y_ref)

    for plane in range(2):
        outs = [ref.at[local, plane].reshape(SLOTS * SUB, LANES) for ref in (keep_ref, send_ref)]
        for js in range(SUB):
            piece = y_ref[pl.ds(js * LANES, LANES), tile(plane)].T
            for half, flat in enumerate(outs):
                flat[pl.ds(js, SLOTS, stride=SUB), :] = piece[half * SLOTS : (half + 1) * SLOTS]


def gather_kernel(first_ref, second_ref, keep_ref, send_ref, *, step):
    left = SLOTS // 2 >> step

    @pl.loop(0, SLOTS // 2, step=SUB)
    def _(at):
        base = 2 * at - at % left if left >= SUB else 2 * at
        for half, ref in enumerate((first_ref, second_ref)):
            for plane in range(2):
                for slot in range(SUB):
                    source = base + (slot if left >= SUB else 2 * slot - slot % left)
                    for side, out in enumerate((keep_ref, send_ref)):
                        out[plane, half * (SLOTS // 2) + at + slot] = ref[plane, source + side * left]


def copies_out(wide_ref, outs, sem, frame):
    return [pltpu.make_async_copy(wide_ref.at[plane], outs[plane].at[frame], sem.at[plane]) for plane in range(2)]


def post_kernel(keep_ref, got_ref, tw_ref, mat_ref, *refs, frame):
    wide_ref, sem, high_ref, low_ref, y_ref = refs[-5:]
    if frame:
        copies = copies_out(refs[0], refs[-7:-5], sem, frame - 1)
        for copy in copies:
            copy.start()
    for plane in range(2):
        flats = [ref.at[plane].reshape(SLOTS * SUB, LANES) for ref in (keep_ref, got_ref)]
        for js in range(SUB):
            pieces = [flat[pl.ds(js, SLOTS, stride=SUB), :] for flat in flats]
            high, low = split(jnp.concatenate(pieces, axis=0).T)
            high_ref[pl.ds(js * LANES, LANES), tile(plane)] = high
            low_ref[pl.ds(js * LANES, LANES), tile(plane)] = low

    matmul3(high_ref, low_ref, mat_ref.at[frame], y_ref)

    @pl.loop(0, 4)
    def _(block):
        at = pl.multiple_of(block * SUB, SUB)

        def load(j):
            row = pl.ds(((j % SUB) * 4 + j // SUB) * SHORT + at, SUB)
            real, imag = y_ref[row, tile(0)], y_ref[row, tile(1)]
            if j:
                c, s = tw_ref[0, pl.ds(j * SUB, SUB), :], tw_ref[1, pl.ds(j * SUB, SUB), :]
                real, imag = real * c - imag * s, real * s + imag * c
            return real, imag

        def store(k, value):
            for plane in range(2):
                wide_ref[plane, pl.ds(at, SUB), tile(k)] = value[plane]

        dft32(load, store)

    if frame:
        for copy in copies:
            copy.wait()


def flush_kernel(wide_ref, *refs):
    for copy in copies_out(wide_ref, refs[-3:-1], refs[-1], FRAMES - 1):
        copy.start()
    for copy in copies_out(wide_ref, refs[-3:-1], refs[-1], FRAMES - 1):
        copy.wait()


VMEM = pl.BlockSpec(memory_space=pltpu.VMEM)
PARAMS = pltpu.CompilerParams(vmem_limit_bytes=12 * 2**20)


def cost(flops):
    return pl.CostEstimate(flops=flops, bytes_accessed=2**21, transcendentals=0)


def matrices(target, source):
    shape = jax.ShapeDtypeStruct((len(ORDERS), 2, 2 * LONG, 2 * LONG), jnp.bfloat16)
    return pl.pallas_call(
        matrix_kernel,
        in_specs=[VMEM] * 3,
        out_specs=[VMEM] * 2,
        out_shape=[shape] * 2,
        compiler_params=PARAMS,
        cost_estimate=cost(10**6),
        name="matrices",
    )(target, source, jnp.asarray(long_matrix()))


def in_hbm(*arrays):
    return [pltpu.with_memory_space_constraint(x, pltpu.HBM) for x in arrays]


def last_rows(real, imag):
    half = jax.ShapeDtypeStruct((2, SUB, N), jnp.float32)
    return pl.pallas_call(
        last_kernel,
        in_specs=[pl.BlockSpec(memory_space=pl.ANY)] * 2,
        out_specs=[VMEM] * 2,
        out_shape=[half] * 2,
        scratch_shapes=[pltpu.VMEM((2, FRAMES, SUB, N), jnp.float32), pltpu.SemaphoreType.DMA((2,))],
        compiler_params=PARAMS,
        cost_estimate=cost(10**6),
        name="last",
    )(*in_hbm(real, imag))


def short(first, count, real, imag, col, tw):
    frame = pl.BlockSpec((1, SHORT, N), lambda f: (first + f, 0, 0))
    return pl.pallas_call(
        short_kernel,
        grid=(count,),
        in_specs=[frame, frame, VMEM, VMEM],
        out_specs=VMEM,
        out_shape=jax.ShapeDtypeStruct((count, 2, ROWS, LANES), jnp.float32),
        compiler_params=pltpu.CompilerParams(vmem_limit_bytes=12 * 2**20),
        cost_estimate=cost(10**9),
    )(*in_hbm(real, imag), col, tw)


def edges(halo, col, tw):
    return pl.pallas_call(
        edge_kernel,
        in_specs=[VMEM] * 3,
        out_specs=VMEM,
        out_shape=jax.ShapeDtypeStruct((2, SHORT * SUB, LANES), jnp.float32),
        compiler_params=PARAMS,
        cost_estimate=cost(10**6),
        name="edges",
    )(halo, col, tw)


def pre(first, count, row, z, edge, mat):
    f32 = jnp.float32
    half = jax.ShapeDtypeStruct((count, 2, SLOTS, SUB, LANES), f32)
    return pl.pallas_call(
        functools.partial(pre_kernel, first=first),
        grid=(count,),
        in_specs=[VMEM] * 4,
        out_specs=[VMEM, VMEM],
        out_shape=[half, half],
        scratch_shapes=[
            pltpu.VMEM((ROWS, 2 * LANES), jnp.bfloat16),
            pltpu.VMEM((ROWS, 2 * LANES), jnp.bfloat16),
            pltpu.VMEM((ROWS, 2 * LANES), f32),
        ],
        compiler_params=PARAMS,
        cost_estimate=cost(5 * 10**8 * count),
    )(row, z, edge, mat)


WIDE = jax.ShapeDtypeStruct((2, SHORT, N), jnp.float32)
OUT = jax.ShapeDtypeStruct((FRAMES, SHORT, N), jnp.float32)
ANY = pl.BlockSpec(memory_space=pl.ANY)


def post(frame, keep, got, tw, mat, before, outs):
    out_shape, out_specs = ([OUT] * 2, [ANY] * 2) if frame else ([], [])
    results = pl.pallas_call(
        functools.partial(post_kernel, frame=frame),
        in_specs=[VMEM] * (5 if frame else 4) + [ANY] * len(outs),
        out_specs=out_specs + [VMEM],
        out_shape=out_shape + [WIDE],
        input_output_aliases={5 + i: i for i in range(len(outs))},
        scratch_shapes=[
            pltpu.SemaphoreType.DMA((2,)),
            pltpu.VMEM((ROWS, 2 * LANES), jnp.bfloat16),
            pltpu.VMEM((ROWS, 2 * LANES), jnp.bfloat16),
            pltpu.VMEM((ROWS, 2 * LANES), jnp.float32),
        ],
        compiler_params=PARAMS,
        cost_estimate=cost(10**9),
    )(keep, got, tw, mat, *([before] if frame else []), *outs)
    return results[-1], tuple(results[:-1])


def flush(wide, outs):
    return pl.pallas_call(
        flush_kernel,
        in_specs=[VMEM] + [ANY] * 2,
        out_specs=[ANY] * 2,
        out_shape=[OUT] * 2,
        input_output_aliases={1: 0, 2: 1},
        scratch_shapes=[pltpu.SemaphoreType.DMA((2,))],
        compiler_params=PARAMS,
        cost_estimate=cost(10**6),
        name="flush",
    )(wide, *outs)


def gather(step, first, second):
    half = jax.ShapeDtypeStruct((2, SLOTS, SUB, LANES), jnp.float32)
    (one, at_one), (two, at_two) = first, second

    def kernel(one_ref, two_ref, keep_ref, send_ref):
        gather_kernel(one_ref.at[at_one], two_ref.at[at_two], keep_ref, send_ref, step=step)

    return pl.pallas_call(
        kernel,
        in_specs=[VMEM] * 2,
        out_specs=[VMEM] * 2,
        out_shape=[half] * 2,
        compiler_params=pltpu.CompilerParams(vmem_limit_bytes=2**20),
        cost_estimate=cost(10**5),
        name="gather",
    )(one, two)


def permute(value, pairs):
    return lax.ppermute(value, "pa", pairs)


def exchange(frame, halves):
    for step in range(STEPS):
        keep, send = gather(step, *halves)
        got = permute(send, edge_pairs(frame, step))
        halves = (keep[None], 0), (got[None], 0)
    return keep, got


def on_device(real, imag):
    frames, rows, _ = real.shape
    me = lax.axis_index("pa")
    halos = [permute(last, [(d, d + 1) for d in range(2 * SLOTS - 1)]) for last in last_rows(real, imag)]
    row = hamming(me * rows + jnp.arange(rows, dtype=jnp.int32)) * (1.0 / (math.sqrt(6.0) * N))
    row = jnp.broadcast_to(row[:, None, None], (rows, SUB, LANES)).reshape(rows * SUB, LANES)
    col = jnp.asarray(column_window())
    tw = jnp.asarray(twiddles())
    z = []
    for first, count in GROUPS:
        z.append(short(first, count, real, imag, col, tw))
    forward, backward = matrices(
        jnp.stack([targets(me, f) for f in range(frames)]),
        jnp.stack([sources(me, f) for f in range(frames)], axis=1),
    )
    edge = [edges(halo, col, tw) for halo in halos]
    halves = []
    for (first, count), part in zip(GROUPS, z):
        keep, send = pre(first, count, row, part, edge[first // 4], forward)
        got = permute(send, [(i, i ^ 1) for i in range(2 * SLOTS)])
        halves += [((keep, i), (got, i)) for i in range(count)]
    ends = [exchange(frame, halves[frame]) for frame in range(frames)]
    wide, outs = None, ()
    for frame in range(frames):
        wide, outs = post(frame, *ends[frame], tw, backward, wide, outs)
    return tuple(flush(wide, outs))


def solution(mesh):
    placed = (P(None, "pa", None), P(None, "pa", None))
    return jax.shard_map(on_device, mesh=mesh, in_specs=placed, out_specs=placed, check_vma=False)
```

```python
import functools
import math

import jax
import jax.numpy as jnp
import numpy as np
from jax import lax
from jax.experimental import pallas as pl
from jax.experimental.pallas import tpu as pltpu
from jax.sharding import PartitionSpec as P


N = 4096
FRAMES = 8
SHORT = 32
LONG = 128
LANES = 128
SUB = 8
ROWS = 4 * SHORT * SUB
ROOT_HALF = math.sqrt(0.5)

EDGES = (4, 2, 0, 5, 3, 1)
ORDERS = (
    ((2, 1, 0, 4, 5, 3), (5, 4, 3, 1, 2, 0)),
    ((1, 0, 2, 5, 3, 4), (4, 3, 5, 2, 0, 1)),
    ((0, 2, 1, 3, 4, 5), (3, 5, 4, 0, 1, 2)),
    ((2, 1, 0, 4, 5, 3), (5, 4, 3, 1, 2, 0)),
    ((1, 0, 2, 5, 3, 4), (4, 3, 5, 2, 0, 1)),
    ((0, 2, 4, 3, 1, 5), (3, 5, 1, 0, 4, 2)),
    ((2, 1, 0, 4, 5, 3), (5, 4, 3, 1, 2, 0)),
    ((0, 1, 2, 3, 5, 4), (3, 4, 5, 0, 2, 1)),
)
STEPS = len(EDGES)
SLOTS = 64
GROUPS = ((0, 2), (2, 2), (4, 2), (6, 2))


def recode(chip):
    return chip ^ (chip >> 1 & 21)


def edges_of(frame, core):
    return [EDGES[e] for e in ORDERS[frame][core]]


def edge_pairs(frame, step):
    pairs = []
    for device in range(2 * SLOTS):
        chip, core = divmod(device, 2)
        partner = recode(recode(chip) ^ (1 << edges_of(frame, core)[step]))
        pairs.append((device, partner * 2 + core))
    return pairs


def peer(me, frame, core_bit, steps):
    core = me % 2 ^ core_bit
    masks = [sum(bit << edge for bit, edge in zip(steps, edges_of(frame, c))) for c in range(2)]
    return recode(recode(me // 2) ^ jnp.where(core == 0, *masks)) * 2 + core


def targets(me, frame):
    slot = jnp.arange(2 * SLOTS, dtype=jnp.int32)
    return peer(me, frame, slot >> STEPS, [slot >> (STEPS - 1 - k) & 1 for k in range(STEPS)])


def sources(me, frame):
    slot = jnp.arange(2 * SLOTS, dtype=jnp.int32)
    masks = [sum((slot >> (k + 1) & 1) << edge for k, edge in enumerate(edges_of(frame, c))) for c in range(2)]
    return recode(recode(me // 2) ^ jnp.where(me % 2 == 0, *masks)) * 2 + (me % 2 ^ slot & 1)


def hamming(index):
    return 0.54 - 0.46 * jnp.cos(index.astype(jnp.float32) * (2.0 * math.pi / N))


def column_window():
    window = 0.54 - 0.46 * np.cos(2.0 * np.pi * np.arange(N) / N)
    return window.astype(np.float32)[None]


def twiddles():
    angle = -2.0 * np.pi * (np.arange(SHORT)[:, None] * np.arange(LONG)[None, :]) / N
    wide = np.repeat(np.stack([np.cos(angle), np.sin(angle)]), SUB, axis=1)
    return wide.astype(np.float32)


def long_matrix():
    phase = np.arange(LONG)[:, None] * np.arange(LONG)[None, :] % LONG
    angle = -2.0 * np.pi * phase / LONG
    real, imag = np.cos(angle), np.sin(angle)
    whole = np.block([[real, imag], [-imag, real]]).astype(np.float32)
    high = whole.astype(jnp.bfloat16)
    return np.stack([high, (whole - high.astype(np.float32)).astype(jnp.bfloat16)])


def add(a, b):
    return a[0] + b[0], a[1] + b[1]


def sub(a, b):
    return a[0] - b[0], a[1] - b[1]


def minus_i(a):
    return a[1], -a[0]


def times(a, angle):
    c, s = math.cos(angle), math.sin(angle)
    return a[0] * c - a[1] * s, a[0] * s + a[1] * c


def rotate(a, power):
    power %= 32
    if power == 0:
        return a
    if power == 8:
        return minus_i(a)
    if power == 4:
        return (a[0] + a[1]) * ROOT_HALF, (a[1] - a[0]) * ROOT_HALF
    if power == 12:
        return (a[1] - a[0]) * ROOT_HALF, (a[0] + a[1]) * -ROOT_HALF
    return times(a, -2.0 * math.pi * power / 32)


def dft4(x):
    s, d = add(x[0], x[2]), sub(x[0], x[2])
    t, e = add(x[1], x[3]), sub(x[1], x[3])
    e = minus_i(e)
    return [add(s, t), add(d, e), sub(s, t), sub(d, e)]


def dft8(x):
    even, odd = dft4(x[0::2]), dft4(x[1::2])
    odd = [rotate(v, 4 * k) for k, v in enumerate(odd)]
    return [add(a, b) for a, b in zip(even, odd)] + [sub(a, b) for a, b in zip(even, odd)]


def dft32(load, store):
    parts = []
    for r in range(4):
        part = dft8([load(4 * i + r) for i in range(8)])
        parts.append([rotate(v, r * k) for k, v in enumerate(part)])
    for k in range(8):
        for q, value in enumerate(dft4([parts[r][k] for r in range(4)])):
            store(k + 8 * q, value)


def split(value):
    high = value.astype(jnp.bfloat16)
    return high, (value - high.astype(jnp.float32)).astype(jnp.bfloat16)


def matmul3(high_ref, low_ref, mat_ref, out_ref):
    dot = functools.partial(jnp.dot, preferred_element_type=jnp.float32)
    high, low = high_ref[...], low_ref[...]
    out_ref[...] = dot(high, mat_ref[0]) + dot(low, mat_ref[0]) + dot(high, mat_ref[1])


def tile(i):
    return pl.ds(i * LANES, LANES)


def short_stage(planes, row0, col_ref, tw_ref, z_ref, z_row):
    def load(a):
        w = col_ref[:, tile(a)]
        return tuple(p[pl.ds(row0, SUB), tile(a)] * w for p in planes)

    def store(k, value):
        real, imag = value
        if k:
            c, s = tw_ref[0, pl.ds(k * SUB, SUB), :], tw_ref[1, pl.ds(k * SUB, SUB), :]
            real, imag = real * c - imag * s, real * s + imag * c
        z_ref[0, pl.ds(z_row + k * SUB, SUB), :] = real
        z_ref[1, pl.ds(z_row + k * SUB, SUB), :] = imag

    dft32(load, store)


def matrix_kernel(target_ref, source_ref, base_ref, forward_ref, backward_ref):
    dot = functools.partial(jnp.dot, preferred_element_type=jnp.float32)
    square = (LONG, LONG)
    for frame in range(len(ORDERS)):
        wanted = jnp.broadcast_to(target_ref[pl.ds(frame, 1), :], square)
        pick = (wanted == lax.broadcasted_iota(jnp.int32, square, 0)).astype(jnp.bfloat16)
        wanted = jnp.broadcast_to(source_ref[:, pl.ds(frame, 1)], square)
        place = (wanted == lax.broadcasted_iota(jnp.int32, square, 1)).astype(jnp.bfloat16)
        for part in range(2):
            for half in range(2):
                forward_ref[frame, part, :, tile(half)] = dot(base_ref[part, :, tile(half)], pick).astype(jnp.bfloat16)
                backward_ref[frame, part, tile(half), :] = dot(place, base_ref[part, tile(half), :]).astype(jnp.bfloat16)


def last_kernel(real_ref, imag_ref, out_a_ref, out_b_ref, rows_ref, sem):
    copies = [
        pltpu.make_async_copy(ref.at[:, pl.ds(SHORT - SUB, SUB)], rows_ref.at[plane], sem.at[plane])
        for plane, ref in enumerate((real_ref, imag_ref))
    ]
    for copy in copies:
        copy.start()
    for plane, copy in enumerate(copies):
        copy.wait()
        for frame in range(FRAMES):
            out = (out_a_ref, out_b_ref)[frame // 4]
            out[plane, pl.ds(frame % 4 * 2, 2), :] = rows_ref[plane, frame, pl.ds(SUB - 2, 2), :]


def short_kernel(real_ref, imag_ref, col_ref, tw_ref, target_ref, source_ref, base_ref, *refs):
    zs, (forward_ref, backward_ref, x_ref, sem) = refs[:-4], refs[-4:]

    def fetch(frame, plane):
        return pltpu.make_async_copy((real_ref, imag_ref)[plane].at[frame], x_ref.at[frame, plane], sem.at[frame, plane])

    for frame in range(FRAMES):
        for plane in range(2):
            fetch(frame, plane).start()

    matrix_kernel(target_ref, source_ref, base_ref, forward_ref, backward_ref)

    for (first, count), z_ref in zip(GROUPS, zs):

        @pl.loop(0, count)
        def _(local):
            frame = first + local
            for plane in range(2):
                fetch(frame, plane).wait()
            planes, z = (x_ref.at[frame, 0], x_ref.at[frame, 1]), z_ref.at[local]

            @pl.loop(0, 4)
            def _(block):
                row = pl.multiple_of(block * SUB, SUB)
                short_stage(planes, row, col_ref, tw_ref, z, pl.multiple_of(row * SHORT, SUB * SHORT))


def edge_kernel(halo_ref, col_ref, tw_ref, out_ref):
    short_stage((halo_ref.at[0], halo_ref.at[1]), 0, col_ref, tw_ref, out_ref, 0)


def pre_kernel(row_ref, z_ref, edge_ref, mat_ref, keep_ref, send_ref, high_ref, low_ref, y_ref, *, first):
    local = pl.program_id(0)
    frame = first + local
    for plane in range(2):

        def rows(js):
            return z_ref[local, plane, pl.ds(js, LANES, stride=SUB), :]

        def rows_before(js):
            edge = edge_ref[plane, pl.ds(frame % 4 * 2 + js - 6, SHORT, stride=SUB), :]
            return jnp.concatenate([edge, z_ref[local, plane, pl.ds(js, 3 * SHORT, stride=SUB), :]], axis=0)

        before = rows_before(7)
        slope = before - rows_before(6)
        for js in range(SUB):
            now = rows(js)
            new_slope = now - before
            value = new_slope - slope
            before, slope = now, new_slope
            for b in range(4):
                part = value[b * SHORT : (b + 1) * SHORT].reshape(SHORT // SUB, SUB, LANES)
                part = part * row_ref[pl.ds((b * SUB + js) * SUB, SUB), :]
                high, low = split(part.reshape(SHORT, LANES))
                high_ref[pl.ds(js * LANES + b * SHORT, SHORT), tile(plane)] = high
                low_ref[pl.ds(js * LANES + b * SHORT, SHORT), tile(plane)] = low

    matmul3(high_ref, low_ref, mat_ref.at[frame], y_ref)

    for plane in range(2):
        outs = [ref.at[local, plane].reshape(SLOTS * SUB, LANES) for ref in (keep_ref, send_ref)]
        for js in range(SUB):
            piece = y_ref[pl.ds(js * LANES, LANES), tile(plane)].T
            for half, flat in enumerate(outs):
                flat[pl.ds(js, SLOTS, stride=SUB), :] = piece[half * SLOTS : (half + 1) * SLOTS]


def gather_kernel(first_ref, second_ref, keep_ref, send_ref, *, step):
    left = SLOTS // 2 >> step

    @pl.loop(0, SLOTS // 2, step=SUB)
    def _(at):
        base = 2 * at - at % left if left >= SUB else 2 * at
        for half, ref in enumerate((first_ref, second_ref)):
            for plane in range(2):
                for slot in range(SUB):
                    source = base + (slot if left >= SUB else 2 * slot - slot % left)
                    for side, out in enumerate((keep_ref, send_ref)):
                        out[plane, half * (SLOTS // 2) + at + slot] = ref[plane, source + side * left]


def copies_out(wide_ref, outs, sem, frame):
    return [pltpu.make_async_copy(wide_ref.at[plane], outs[plane].at[frame], sem.at[plane]) for plane in range(2)]


def post_kernel(keep_ref, got_ref, tw_ref, mat_ref, *refs, frame):
    wide_ref, sem, high_ref, low_ref, y_ref = refs[-5:]
    if frame:
        copies = copies_out(refs[0], refs[-7:-5], sem, frame - 1)
        for copy in copies:
            copy.start()
    for plane in range(2):
        flats = [ref.at[plane].reshape(SLOTS * SUB, LANES) for ref in (keep_ref, got_ref)]
        for js in range(SUB):
            pieces = [flat[pl.ds(js, SLOTS, stride=SUB), :] for flat in flats]
            high, low = split(jnp.concatenate(pieces, axis=0).T)
            high_ref[pl.ds(js * LANES, LANES), tile(plane)] = high
            low_ref[pl.ds(js * LANES, LANES), tile(plane)] = low

    matmul3(high_ref, low_ref, mat_ref.at[frame], y_ref)

    @pl.loop(0, 4)
    def _(block):
        at = pl.multiple_of(block * SUB, SUB)

        def load(j):
            row = pl.ds(((j % SUB) * 4 + j // SUB) * SHORT + at, SUB)
            real, imag = y_ref[row, tile(0)], y_ref[row, tile(1)]
            if j:
                c, s = tw_ref[0, pl.ds(j * SUB, SUB), :], tw_ref[1, pl.ds(j * SUB, SUB), :]
                real, imag = real * c - imag * s, real * s + imag * c
            return real, imag

        def store(k, value):
            for plane in range(2):
                wide_ref[plane, pl.ds(at, SUB), tile(k)] = value[plane]

        dft32(load, store)

    if frame:
        for copy in copies:
            copy.wait()


def flush_kernel(wide_ref, *refs):
    for copy in copies_out(wide_ref, refs[-3:-1], refs[-1], FRAMES - 1):
        copy.start()
    for copy in copies_out(wide_ref, refs[-3:-1], refs[-1], FRAMES - 1):
        copy.wait()


VMEM = pl.BlockSpec(memory_space=pltpu.VMEM)
ANY = pl.BlockSpec(memory_space=pl.ANY)
PARAMS = pltpu.CompilerParams(vmem_limit_bytes=12 * 2**20)


def cost(flops):
    return pl.CostEstimate(flops=flops, bytes_accessed=2**21, transcendentals=0)


def in_hbm(*arrays):
    return [pltpu.with_memory_space_constraint(x, pltpu.HBM) for x in arrays]


def last_rows(real, imag):
    half = jax.ShapeDtypeStruct((2, SUB, N), jnp.float32)
    return pl.pallas_call(
        last_kernel,
        in_specs=[ANY] * 2,
        out_specs=[VMEM] * 2,
        out_shape=[half] * 2,
        scratch_shapes=[pltpu.VMEM((2, FRAMES, SUB, N), jnp.float32), pltpu.SemaphoreType.DMA((2,))],
        compiler_params=PARAMS,
        cost_estimate=cost(10**6),
        name="last",
    )(*in_hbm(real, imag))


def short(real, imag, col, tw, target, source):
    matrix = jax.ShapeDtypeStruct((FRAMES, 2, 2 * LONG, 2 * LONG), jnp.bfloat16)
    *zs, forward, backward = pl.pallas_call(
        short_kernel,
        in_specs=[ANY] * 2 + [VMEM] * 5,
        out_specs=[VMEM] * (len(GROUPS) + 2),
        out_shape=[jax.ShapeDtypeStruct((count, 2, ROWS, LANES), jnp.float32) for _, count in GROUPS] + [matrix] * 2,
        scratch_shapes=[pltpu.VMEM((FRAMES, 2, SHORT, N), jnp.float32), pltpu.SemaphoreType.DMA((FRAMES, 2))],
        compiler_params=PARAMS,
        cost_estimate=cost(10**9),
        name="short",
    )(*in_hbm(real, imag), col, tw, target, source, jnp.asarray(long_matrix()))
    return zs, forward, backward


def edges(halo, col, tw):
    return pl.pallas_call(
        edge_kernel,
        in_specs=[VMEM] * 3,
        out_specs=VMEM,
        out_shape=jax.ShapeDtypeStruct((2, SHORT * SUB, LANES), jnp.float32),
        compiler_params=PARAMS,
        cost_estimate=cost(10**6),
        name="edges",
    )(halo, col, tw)


def pre(first, count, row, z, edge, mat):
    f32 = jnp.float32
    half = jax.ShapeDtypeStruct((count, 2, SLOTS, SUB, LANES), f32)
    return pl.pallas_call(
        functools.partial(pre_kernel, first=first),
        grid=(count,),
        in_specs=[VMEM] * 4,
        out_specs=[VMEM, VMEM],
        out_shape=[half, half],
        scratch_shapes=[
            pltpu.VMEM((ROWS, 2 * LANES), jnp.bfloat16),
            pltpu.VMEM((ROWS, 2 * LANES), jnp.bfloat16),
            pltpu.VMEM((ROWS, 2 * LANES), f32),
        ],
        compiler_params=PARAMS,
        cost_estimate=cost(5 * 10**8 * count),
    )(row, z, edge, mat)


WIDE = jax.ShapeDtypeStruct((2, SHORT, N), jnp.float32)
OUT = jax.ShapeDtypeStruct((FRAMES, SHORT, N), jnp.float32)


def post(frame, keep, got, tw, mat, before, outs):
    out_shape, out_specs = ([OUT] * 2, [ANY] * 2) if frame else ([], [])
    results = pl.pallas_call(
        functools.partial(post_kernel, frame=frame),
        in_specs=[VMEM] * (5 if frame else 4) + [ANY] * len(outs),
        out_specs=out_specs + [VMEM],
        out_shape=out_shape + [WIDE],
        input_output_aliases={5 + i: i for i in range(len(outs))},
        scratch_shapes=[
            pltpu.SemaphoreType.DMA((2,)),
            pltpu.VMEM((ROWS, 2 * LANES), jnp.bfloat16),
            pltpu.VMEM((ROWS, 2 * LANES), jnp.bfloat16),
            pltpu.VMEM((ROWS, 2 * LANES), jnp.float32),
        ],
        compiler_params=PARAMS,
        cost_estimate=cost(10**9),
    )(keep, got, tw, mat, *([before] if frame else []), *outs)
    return results[-1], tuple(results[:-1])


def flush(wide, outs):
    return pl.pallas_call(
        flush_kernel,
        in_specs=[VMEM] + [ANY] * 2,
        out_specs=[ANY] * 2,
        out_shape=[OUT] * 2,
        input_output_aliases={1: 0, 2: 1},
        scratch_shapes=[pltpu.SemaphoreType.DMA((2,))],
        compiler_params=PARAMS,
        cost_estimate=cost(10**6),
        name="flush",
    )(wide, *outs)


def gather(step, first, second):
    half = jax.ShapeDtypeStruct((2, SLOTS, SUB, LANES), jnp.float32)
    (one, at_one), (two, at_two) = first, second

    def kernel(one_ref, two_ref, keep_ref, send_ref):
        gather_kernel(one_ref.at[at_one], two_ref.at[at_two], keep_ref, send_ref, step=step)

    return pl.pallas_call(
        kernel,
        in_specs=[VMEM] * 2,
        out_specs=[VMEM] * 2,
        out_shape=[half] * 2,
        compiler_params=pltpu.CompilerParams(vmem_limit_bytes=2**20),
        cost_estimate=cost(10**5),
        name="gather",
    )(one, two)


def permute(value, pairs):
    return lax.ppermute(value, "pa", pairs)


def exchange(frame, halves):
    for step in range(STEPS):
        keep, send = gather(step, *halves)
        got = permute(send, edge_pairs(frame, step))
        halves = (keep[None], 0), (got[None], 0)
    return keep, got


def on_device(real, imag):
    frames, rows, _ = real.shape
    me = lax.axis_index("pa")
    halos = [permute(last, [(d, d + 1) for d in range(2 * SLOTS - 1)]) for last in last_rows(real, imag)]
    row = hamming(me * rows + jnp.arange(rows, dtype=jnp.int32)) * (1.0 / (math.sqrt(6.0) * N))
    row = jnp.broadcast_to(row[:, None, None], (rows, SUB, LANES)).reshape(rows * SUB, LANES)
    col = jnp.asarray(column_window())
    tw = jnp.asarray(twiddles())
    target = jnp.stack([targets(me, f) for f in range(frames)])
    source = jnp.stack([sources(me, f) for f in range(frames)], axis=1)
    z, forward, backward = short(real, imag, col, tw, target, source)
    edge = [edges(halo, col, tw) for halo in halos]
    halves = []
    for (first, count), part in zip(GROUPS, z):
        keep, send = pre(first, count, row, part, edge[first // 4], forward)
        got = permute(send, [(i, i ^ 1) for i in range(2 * SLOTS)])
        halves += [((keep, i), (got, i)) for i in range(count)]
    ends = [exchange(frame, halves[frame]) for frame in range(frames)]
    wide, outs = None, ()
    for frame in range(frames):
        wide, outs = post(frame, *ends[frame], tw, backward, wide, outs)
    return tuple(flush(wide, outs))


def solution(mesh):
    placed = (P(None, "pa", None), P(None, "pa", None))
    return jax.shard_map(on_device, mesh=mesh, in_specs=placed, out_specs=placed, check_vma=False)
```

```python
import functools
import math

import jax
import jax.numpy as jnp
import numpy as np
from jax import lax
from jax.experimental import pallas as pl
from jax.experimental.pallas import tpu as pltpu
from jax.sharding import PartitionSpec as P


N = 4096
FRAMES = 8
SHORT = 32
LONG = 128
LANES = 128
SUB = 8
ROWS = 4 * SHORT * SUB
ROOT_HALF = math.sqrt(0.5)

EDGES = (4, 2, 0, 5, 3, 1)
ORDERS = (
    ((0, 2, 3, 4, 1, 5), (3, 5, 0, 1, 4, 2)),
    ((1, 3, 4, 5, 2, 0), (4, 0, 1, 2, 5, 3)),
    ((2, 1, 3, 4, 5, 0), (5, 4, 0, 1, 2, 3)),
    ((1, 2, 0, 3, 4, 5), (4, 5, 3, 0, 1, 2)),
    ((3, 5, 2, 0, 4, 1), (0, 2, 5, 3, 1, 4)),
    ((2, 0, 3, 4, 1, 5), (5, 3, 0, 1, 4, 2)),
    ((1, 4, 2, 3, 5, 0), (4, 1, 5, 0, 2, 3)),
    ((4, 5, 3, 0, 1, 2), (1, 2, 0, 3, 4, 5)),
)
STEPS = len(EDGES)
SLOTS = 64
GROUPS = ((0, 2), (2, 2), (4, 2), (6, 2))


LATE = (0, 1, 2, 3)
CORES = [(d, d ^ 1) for d in range(2 * SLOTS)]


def recode(chip):
    return chip ^ (chip >> 1 & 21)


def edges_of(frame, core):
    return [EDGES[e] for e in ORDERS[frame][core]]


def edge_pairs(frame, step):
    pairs = []
    for device in range(2 * SLOTS):
        chip, core = divmod(device, 2)
        partner = recode(recode(chip) ^ (1 << edges_of(frame, core)[step]))
        pairs.append((device, partner * 2 + core))
    return pairs


def peer(me, frame, core, traveller, steps):
    masks = [sum(bit << edge for bit, edge in zip(steps, edges_of(frame, c))) for c in range(2)]
    return recode(recode(me // 2) ^ jnp.where(traveller == 0, *masks)) * 2 + core


def targets(me, frame):
    slot = jnp.arange(2 * SLOTS, dtype=jnp.int32)
    core = me % 2 ^ slot >> STEPS
    steps = [slot >> (STEPS - 1 - k) & 1 for k in range(STEPS)]
    return peer(me, frame, core, me % 2 if frame in LATE else core, steps)


def sources(me, frame):
    slot = jnp.arange(2 * SLOTS, dtype=jnp.int32)
    if frame in LATE:
        core = me % 2 ^ slot >> STEPS
        return peer(me, frame, core, core, [slot >> k & 1 for k in range(STEPS)])
    return peer(me, frame, me % 2 ^ slot & 1, me % 2, [slot >> (k + 1) & 1 for k in range(STEPS)])


def hamming(index):
    return 0.54 - 0.46 * jnp.cos(index.astype(jnp.float32) * (2.0 * math.pi / N))


def column_window():
    window = 0.54 - 0.46 * np.cos(2.0 * np.pi * np.arange(N) / N)
    return window.astype(np.float32)[None]


def twiddles():
    angle = -2.0 * np.pi * (np.arange(SHORT)[:, None] * np.arange(LONG)[None, :]) / N
    wide = np.repeat(np.stack([np.cos(angle), np.sin(angle)]), SUB, axis=1)
    return wide.astype(np.float32)


def long_matrix():
    phase = np.arange(LONG)[:, None] * np.arange(LONG)[None, :] % LONG
    angle = -2.0 * np.pi * phase / LONG
    real, imag = np.cos(angle), np.sin(angle)
    whole = np.block([[real, imag], [-imag, real]]).astype(np.float32)
    high = whole.astype(jnp.bfloat16)
    return np.stack([high, (whole - high.astype(np.float32)).astype(jnp.bfloat16)])


def add(a, b):
    return a[0] + b[0], a[1] + b[1]


def sub(a, b):
    return a[0] - b[0], a[1] - b[1]


def minus_i(a):
    return a[1], -a[0]


def times(a, angle):
    c, s = math.cos(angle), math.sin(angle)
    return a[0] * c - a[1] * s, a[0] * s + a[1] * c


def rotate(a, power):
    power %= 32
    if power == 0:
        return a
    if power == 8:
        return minus_i(a)
    if power == 4:
        return (a[0] + a[1]) * ROOT_HALF, (a[1] - a[0]) * ROOT_HALF
    if power == 12:
        return (a[1] - a[0]) * ROOT_HALF, (a[0] + a[1]) * -ROOT_HALF
    return times(a, -2.0 * math.pi * power / 32)


def dft4(x):
    s, d = add(x[0], x[2]), sub(x[0], x[2])
    t, e = add(x[1], x[3]), sub(x[1], x[3])
    e = minus_i(e)
    return [add(s, t), add(d, e), sub(s, t), sub(d, e)]


def dft8(x):
    even, odd = dft4(x[0::2]), dft4(x[1::2])
    odd = [rotate(v, 4 * k) for k, v in enumerate(odd)]
    return [add(a, b) for a, b in zip(even, odd)] + [sub(a, b) for a, b in zip(even, odd)]


def dft32(load, store):
    parts = []
    for r in range(4):
        part = dft8([load(4 * i + r) for i in range(8)])
        parts.append([rotate(v, r * k) for k, v in enumerate(part)])
    for k in range(8):
        for q, value in enumerate(dft4([parts[r][k] for r in range(4)])):
            store(k + 8 * q, value)


def split(value):
    high = value.astype(jnp.bfloat16)
    return high, (value - high.astype(jnp.float32)).astype(jnp.bfloat16)


def matmul3(high_ref, low_ref, mat_ref, out_ref):
    dot = functools.partial(jnp.dot, preferred_element_type=jnp.float32)
    high, low = high_ref[...], low_ref[...]
    out_ref[...] = dot(high, mat_ref[0]) + dot(low, mat_ref[0]) + dot(high, mat_ref[1])


def tile(i):
    return pl.ds(i * LANES, LANES)


def short_stage(planes, row0, col_ref, tw_ref, z_ref, z_row):
    def load(a):
        w = col_ref[:, tile(a)]
        return tuple(p[pl.ds(row0, SUB), tile(a)] * w for p in planes)

    def store(k, value):
        real, imag = value
        if k:
            c, s = tw_ref[0, pl.ds(k * SUB, SUB), :], tw_ref[1, pl.ds(k * SUB, SUB), :]
            real, imag = real * c - imag * s, real * s + imag * c
        z_ref[0, pl.ds(z_row + k * SUB, SUB), :] = real
        z_ref[1, pl.ds(z_row + k * SUB, SUB), :] = imag

    dft32(load, store)


def matrix_kernel(target_ref, source_ref, base_ref, forward_ref, backward_ref):
    dot = functools.partial(jnp.dot, preferred_element_type=jnp.float32)
    square = (LONG, LONG)
    for frame in range(len(ORDERS)):
        wanted = jnp.broadcast_to(target_ref[pl.ds(frame, 1), :], square)
        pick = (wanted == lax.broadcasted_iota(jnp.int32, square, 0)).astype(jnp.bfloat16)
        wanted = jnp.broadcast_to(source_ref[:, pl.ds(frame, 1)], square)
        place = (wanted == lax.broadcasted_iota(jnp.int32, square, 1)).astype(jnp.bfloat16)
        for part in range(2):
            for half in range(2):
                forward_ref[frame, part, :, tile(half)] = dot(base_ref[part, :, tile(half)], pick).astype(jnp.bfloat16)
                backward_ref[frame, part, tile(half), :] = dot(place, base_ref[part, tile(half), :]).astype(jnp.bfloat16)


def last_kernel(real_ref, imag_ref, out_a_ref, out_b_ref, rows_ref, sem):
    copies = [
        pltpu.make_async_copy(ref.at[:, pl.ds(SHORT - SUB, SUB)], rows_ref.at[plane], sem.at[plane])
        for plane, ref in enumerate((real_ref, imag_ref))
    ]
    for copy in copies:
        copy.start()
    for plane, copy in enumerate(copies):
        copy.wait()
        for frame in range(FRAMES):
            out = (out_a_ref, out_b_ref)[frame // 4]
            out[plane, pl.ds(frame % 4 * 2, 2), :] = rows_ref[plane, frame, pl.ds(SUB - 2, 2), :]


def short_kernel(real_ref, imag_ref, col_ref, tw_ref, target_ref, source_ref, base_ref, *refs):
    zs, (forward_ref, backward_ref, x_ref, sem) = refs[:-4], refs[-4:]

    def fetch(frame, plane):
        return pltpu.make_async_copy((real_ref, imag_ref)[plane].at[frame], x_ref.at[frame, plane], sem.at[frame, plane])

    for frame in range(FRAMES):
        for plane in range(2):
            fetch(frame, plane).start()

    matrix_kernel(target_ref, source_ref, base_ref, forward_ref, backward_ref)

    for (first, count), z_ref in zip(GROUPS, zs):

        @pl.loop(0, count)
        def _(local):
            frame = first + local
            for plane in range(2):
                fetch(frame, plane).wait()
            planes, z = (x_ref.at[frame, 0], x_ref.at[frame, 1]), z_ref.at[local]

            @pl.loop(0, 4)
            def _(block):
                row = pl.multiple_of(block * SUB, SUB)
                short_stage(planes, row, col_ref, tw_ref, z, pl.multiple_of(row * SHORT, SUB * SHORT))


def edge_kernel(halo_ref, col_ref, tw_ref, out_ref):
    short_stage((halo_ref.at[0], halo_ref.at[1]), 0, col_ref, tw_ref, out_ref, 0)


def pre_kernel(row_ref, z_ref, edge_ref, mat_ref, keep_ref, send_ref, high_ref, low_ref, y_ref, *, first):
    local = pl.program_id(0)
    frame = first + local
    for plane in range(2):

        def rows(js):
            return z_ref[local, plane, pl.ds(js, LANES, stride=SUB), :]

        def rows_before(js):
            edge = edge_ref[plane, pl.ds(frame % 4 * 2 + js - 6, SHORT, stride=SUB), :]
            return jnp.concatenate([edge, z_ref[local, plane, pl.ds(js, 3 * SHORT, stride=SUB), :]], axis=0)

        before = rows_before(7)
        slope = before - rows_before(6)
        for js in range(SUB):
            now = rows(js)
            new_slope = now - before
            value = new_slope - slope
            before, slope = now, new_slope
            for b in range(4):
                part = value[b * SHORT : (b + 1) * SHORT].reshape(SHORT // SUB, SUB, LANES)
                part = part * row_ref[pl.ds((b * SUB + js) * SUB, SUB), :]
                high, low = split(part.reshape(SHORT, LANES))
                high_ref[pl.ds(js * LANES + b * SHORT, SHORT), tile(plane)] = high
                low_ref[pl.ds(js * LANES + b * SHORT, SHORT), tile(plane)] = low

    matmul3(high_ref, low_ref, mat_ref.at[frame], y_ref)

    for plane in range(2):
        outs = [ref.at[local, plane].reshape(SLOTS * SUB, LANES) for ref in (keep_ref, send_ref)]
        for js in range(SUB):
            piece = y_ref[pl.ds(js * LANES, LANES), tile(plane)].T
            for half, flat in enumerate(outs):
                flat[pl.ds(js, SLOTS, stride=SUB), :] = piece[half * SLOTS : (half + 1) * SLOTS]


def gather_kernel(first_ref, second_ref, keep_ref, send_ref, *, step):
    left = SLOTS // 2 >> step

    @pl.loop(0, SLOTS // 2, step=SUB)
    def _(at):
        base = 2 * at - at % left if left >= SUB else 2 * at
        for half, ref in enumerate((first_ref, second_ref)):
            for plane in range(2):
                for slot in range(SUB):
                    source = base + (slot if left >= SUB else 2 * slot - slot % left)
                    for side, out in enumerate((keep_ref, send_ref)):
                        out[plane, half * (SLOTS // 2) + at + slot] = ref[plane, source + side * left]


def copies_out(wide_ref, outs, sem, frame):
    return [pltpu.make_async_copy(wide_ref.at[plane], outs[plane].at[frame], sem.at[plane]) for plane in range(2)]


def post_kernel(keep_ref, got_ref, tw_ref, mat_ref, *refs, frame):
    wide_ref, sem, high_ref, low_ref, y_ref = refs[-5:]
    if frame:
        copies = copies_out(refs[0], refs[-7:-5], sem, frame - 1)
        for copy in copies:
            copy.start()
    for plane in range(2):
        flats = [ref.at[plane].reshape(SLOTS * SUB, LANES) for ref in (keep_ref, got_ref)]
        for js in range(SUB):
            pieces = [flat[pl.ds(js, SLOTS, stride=SUB), :] for flat in flats]
            high, low = split(jnp.concatenate(pieces, axis=0).T)
            high_ref[pl.ds(js * LANES, LANES), tile(plane)] = high
            low_ref[pl.ds(js * LANES, LANES), tile(plane)] = low

    matmul3(high_ref, low_ref, mat_ref.at[frame], y_ref)

    @pl.loop(0, 4)
    def _(block):
        at = pl.multiple_of(block * SUB, SUB)

        def load(j):
            row = pl.ds(((j % SUB) * 4 + j // SUB) * SHORT + at, SUB)
            real, imag = y_ref[row, tile(0)], y_ref[row, tile(1)]
            if j:
                c, s = tw_ref[0, pl.ds(j * SUB, SUB), :], tw_ref[1, pl.ds(j * SUB, SUB), :]
                real, imag = real * c - imag * s, real * s + imag * c
            return real, imag

        def store(k, value):
            for plane in range(2):
                wide_ref[plane, pl.ds(at, SUB), tile(k)] = value[plane]

        dft32(load, store)

    if frame:
        for copy in copies:
            copy.wait()


def flush_kernel(wide_ref, *refs):
    for copy in copies_out(wide_ref, refs[-3:-1], refs[-1], FRAMES - 1):
        copy.start()
    for copy in copies_out(wide_ref, refs[-3:-1], refs[-1], FRAMES - 1):
        copy.wait()


VMEM = pl.BlockSpec(memory_space=pltpu.VMEM)
ANY = pl.BlockSpec(memory_space=pl.ANY)
PARAMS = pltpu.CompilerParams(vmem_limit_bytes=12 * 2**20)


def cost(flops):
    return pl.CostEstimate(flops=flops, bytes_accessed=2**21, transcendentals=0)


def in_hbm(*arrays):
    return [pltpu.with_memory_space_constraint(x, pltpu.HBM) for x in arrays]


def last_rows(real, imag):
    half = jax.ShapeDtypeStruct((2, SUB, N), jnp.float32)
    return pl.pallas_call(
        last_kernel,
        in_specs=[ANY] * 2,
        out_specs=[VMEM] * 2,
        out_shape=[half] * 2,
        scratch_shapes=[pltpu.VMEM((2, FRAMES, SUB, N), jnp.float32), pltpu.SemaphoreType.DMA((2,))],
        compiler_params=PARAMS,
        cost_estimate=cost(10**6),
        name="last",
    )(*in_hbm(real, imag))


def short(real, imag, col, tw, target, source):
    matrix = jax.ShapeDtypeStruct((FRAMES, 2, 2 * LONG, 2 * LONG), jnp.bfloat16)
    *zs, forward, backward = pl.pallas_call(
        short_kernel,
        in_specs=[ANY] * 2 + [VMEM] * 5,
        out_specs=[VMEM] * (len(GROUPS) + 2),
        out_shape=[jax.ShapeDtypeStruct((count, 2, ROWS, LANES), jnp.float32) for _, count in GROUPS] + [matrix] * 2,
        scratch_shapes=[pltpu.VMEM((FRAMES, 2, SHORT, N), jnp.float32), pltpu.SemaphoreType.DMA((FRAMES, 2))],
        compiler_params=PARAMS,
        cost_estimate=cost(10**9),
        name="short",
    )(*in_hbm(real, imag), col, tw, target, source, jnp.asarray(long_matrix()))
    return zs, forward, backward


def edges(halo, col, tw):
    return pl.pallas_call(
        edge_kernel,
        in_specs=[VMEM] * 3,
        out_specs=VMEM,
        out_shape=jax.ShapeDtypeStruct((2, SHORT * SUB, LANES), jnp.float32),
        compiler_params=PARAMS,
        cost_estimate=cost(10**6),
        name="edges",
    )(halo, col, tw)


def pre(first, count, row, z, edge, mat):
    f32 = jnp.float32
    half = jax.ShapeDtypeStruct((count, 2, SLOTS, SUB, LANES), f32)
    return pl.pallas_call(
        functools.partial(pre_kernel, first=first),
        grid=(count,),
        in_specs=[VMEM] * 4,
        out_specs=[VMEM, VMEM],
        out_shape=[half, half],
        scratch_shapes=[
            pltpu.VMEM((ROWS, 2 * LANES), jnp.bfloat16),
            pltpu.VMEM((ROWS, 2 * LANES), jnp.bfloat16),
            pltpu.VMEM((ROWS, 2 * LANES), f32),
        ],
        compiler_params=PARAMS,
        cost_estimate=cost(5 * 10**8 * count),
    )(row, z, edge, mat)


WIDE = jax.ShapeDtypeStruct((2, SHORT, N), jnp.float32)
OUT = jax.ShapeDtypeStruct((FRAMES, SHORT, N), jnp.float32)


def post(frame, keep, got, tw, mat, before, outs):
    out_shape, out_specs = ([OUT] * 2, [ANY] * 2) if frame else ([], [])
    results = pl.pallas_call(
        functools.partial(post_kernel, frame=frame),
        in_specs=[VMEM] * (5 if frame else 4) + [ANY] * len(outs),
        out_specs=out_specs + [VMEM],
        out_shape=out_shape + [WIDE],
        input_output_aliases={5 + i: i for i in range(len(outs))},
        scratch_shapes=[
            pltpu.SemaphoreType.DMA((2,)),
            pltpu.VMEM((ROWS, 2 * LANES), jnp.bfloat16),
            pltpu.VMEM((ROWS, 2 * LANES), jnp.bfloat16),
            pltpu.VMEM((ROWS, 2 * LANES), jnp.float32),
        ],
        compiler_params=PARAMS,
        cost_estimate=cost(10**9),
    )(keep, got, tw, mat, *([before] if frame else []), *outs)
    return results[-1], tuple(results[:-1])


def flush(wide, outs):
    return pl.pallas_call(
        flush_kernel,
        in_specs=[VMEM] + [ANY] * 2,
        out_specs=[ANY] * 2,
        out_shape=[OUT] * 2,
        input_output_aliases={1: 0, 2: 1},
        scratch_shapes=[pltpu.SemaphoreType.DMA((2,))],
        compiler_params=PARAMS,
        cost_estimate=cost(10**6),
        name="flush",
    )(wide, *outs)


def gather(step, first, second):
    half = jax.ShapeDtypeStruct((2, SLOTS, SUB, LANES), jnp.float32)
    (one, at_one), (two, at_two) = first, second

    def kernel(one_ref, two_ref, keep_ref, send_ref):
        gather_kernel(one_ref.at[at_one], two_ref.at[at_two], keep_ref, send_ref, step=step)

    return pl.pallas_call(
        kernel,
        in_specs=[VMEM] * 2,
        out_specs=[VMEM] * 2,
        out_shape=[half] * 2,
        compiler_params=pltpu.CompilerParams(vmem_limit_bytes=2**20),
        cost_estimate=cost(10**5),
        name="gather",
    )(one, two)


def permute(value, pairs):
    return lax.ppermute(value, "pa", pairs)


def exchange(frame, halves):
    for step in range(STEPS):
        keep, send = gather(step, *halves)
        got = permute(send, edge_pairs(frame, step))
        halves = (keep[None], 0), (got[None], 0)
    if frame in LATE:
        keep, send = gather(STEPS - 1, *halves)
        got = permute(send, CORES)
    return keep, got


def on_device(real, imag):
    frames, rows, _ = real.shape
    me = lax.axis_index("pa")
    halos = [permute(last, [(d, d + 1) for d in range(2 * SLOTS - 1)]) for last in last_rows(real, imag)]
    row = hamming(me * rows + jnp.arange(rows, dtype=jnp.int32)) * (1.0 / (math.sqrt(6.0) * N))
    row = jnp.broadcast_to(row[:, None, None], (rows, SUB, LANES)).reshape(rows * SUB, LANES)
    col = jnp.asarray(column_window())
    tw = jnp.asarray(twiddles())
    target = jnp.stack([targets(me, f) for f in range(frames)])
    source = jnp.stack([sources(me, f) for f in range(frames)], axis=1)
    z, forward, backward = short(real, imag, col, tw, target, source)
    edge = [edges(halo, col, tw) for halo in halos]
    halves = []
    for (first, count), part in zip(GROUPS, z):
        keep, send = pre(first, count, row, part, edge[first // 4], forward)
        if first not in LATE:
            send = permute(send, CORES)
        halves += [((keep, i), (send, i)) for i in range(count)]
    ends = [exchange(frame, halves[frame]) for frame in range(frames)]
    wide, outs = None, ()
    for frame in range(frames):
        wide, outs = post(frame, *ends[frame], tw, backward, wide, outs)
    return tuple(flush(wide, outs))


def solution(mesh):
    placed = (P(None, "pa", None), P(None, "pa", None))
    return jax.shard_map(on_device, mesh=mesh, in_specs=placed, out_specs=placed, check_vma=False)
```

```python
import functools
import math

import jax
import jax.numpy as jnp
import numpy as np
from jax import lax
from jax.experimental import pallas as pl
from jax.experimental.pallas import tpu as pltpu
from jax.sharding import PartitionSpec as P


N = 4096
FRAMES = 8
SHORT = 32
LONG = 128
LANES = 128
SUB = 8
ROWS = 4 * SHORT * SUB
ROOT_HALF = math.sqrt(0.5)

EDGES = (4, 2, 0, 5, 3, 1)
ORDERS = (
    ((0, 2, 3, 4, 1, 5), (3, 5, 0, 1, 4, 2)),
    ((1, 3, 4, 5, 2, 0), (4, 0, 1, 2, 5, 3)),
    ((2, 1, 3, 4, 5, 0), (5, 4, 0, 1, 2, 3)),
    ((1, 2, 0, 3, 4, 5), (4, 5, 3, 0, 1, 2)),
    ((3, 5, 2, 0, 4, 1), (0, 2, 5, 3, 1, 4)),
    ((2, 0, 3, 4, 1, 5), (5, 3, 0, 1, 4, 2)),
    ((1, 4, 2, 3, 5, 0), (4, 1, 5, 0, 2, 3)),
    ((4, 5, 3, 0, 1, 2), (1, 2, 0, 3, 4, 5)),
)
STEPS = len(EDGES)
SLOTS = 64
GROUPS = ((0, 2), (2, 2), (4, 2), (6, 2))


LATE = (0, 1, 2, 3)
CORES = [(d, d ^ 1) for d in range(2 * SLOTS)]


def recode(chip):
    return chip ^ (chip >> 1 & 21)


def edges_of(frame, core):
    return [EDGES[e] for e in ORDERS[frame][core]]


def edge_pairs(frame, step):
    pairs = []
    for device in range(2 * SLOTS):
        chip, core = divmod(device, 2)
        partner = recode(recode(chip) ^ (1 << edges_of(frame, core)[step]))
        pairs.append((device, partner * 2 + core))
    return pairs


def routes(forward):
    slot = np.arange(2 * SLOTS)
    masks, other = np.zeros((2, FRAMES, 2 * SLOTS), np.int32), np.zeros((FRAMES, 2 * SLOTS), np.int32)
    for frame in range(FRAMES):
        late = frame in LATE
        other[frame] = slot >> STEPS if forward or late else slot & 1
        for core in range(2):
            if forward:
                traveller = core + 0 * slot if late else core ^ other[frame]
            else:
                traveller = core ^ other[frame] if late else core + 0 * slot
            for k in range(STEPS):
                place = STEPS - 1 - k if forward else k if late else k + 1
                edge = np.where(traveller == 0, edges_of(frame, 0)[k], edges_of(frame, 1)[k])
                masks[core, frame] |= (slot >> place & 1) << edge
    return (masks, other) if forward else (masks.transpose(0, 2, 1), other.T)


def devices(me, forward):
    masks, other = routes(forward)
    mask = jnp.where(me % 2 == 0, jnp.asarray(masks[0]), jnp.asarray(masks[1]))
    return recode(recode(me // 2) ^ mask) * 2 + (me % 2 ^ jnp.asarray(other))


def hamming(index):
    return 0.54 - 0.46 * jnp.cos(index.astype(jnp.float32) * (2.0 * math.pi / N))


def column_window():
    window = 0.54 - 0.46 * np.cos(2.0 * np.pi * np.arange(N) / N)
    return window.astype(np.float32)[None]


def twiddles():
    angle = -2.0 * np.pi * (np.arange(SHORT)[:, None] * np.arange(LONG)[None, :]) / N
    wide = np.repeat(np.stack([np.cos(angle), np.sin(angle)]), SUB, axis=1)
    return wide.astype(np.float32)


def long_matrix():
    phase = np.arange(LONG)[:, None] * np.arange(LONG)[None, :] % LONG
    angle = -2.0 * np.pi * phase / LONG
    real, imag = np.cos(angle), np.sin(angle)
    whole = np.block([[real, imag], [-imag, real]]).astype(np.float32)
    high = whole.astype(jnp.bfloat16)
    return np.stack([high, (whole - high.astype(np.float32)).astype(jnp.bfloat16)])


def add(a, b):
    return a[0] + b[0], a[1] + b[1]


def sub(a, b):
    return a[0] - b[0], a[1] - b[1]


def minus_i(a):
    return a[1], -a[0]


def times(a, angle):
    c, s = math.cos(angle), math.sin(angle)
    return a[0] * c - a[1] * s, a[0] * s + a[1] * c


def rotate(a, power):
    power %= 32
    if power == 0:
        return a
    if power == 8:
        return minus_i(a)
    if power == 4:
        return (a[0] + a[1]) * ROOT_HALF, (a[1] - a[0]) * ROOT_HALF
    if power == 12:
        return (a[1] - a[0]) * ROOT_HALF, (a[0] + a[1]) * -ROOT_HALF
    return times(a, -2.0 * math.pi * power / 32)


def dft4(x):
    s, d = add(x[0], x[2]), sub(x[0], x[2])
    t, e = add(x[1], x[3]), sub(x[1], x[3])
    e = minus_i(e)
    return [add(s, t), add(d, e), sub(s, t), sub(d, e)]


def dft8(x):
    even, odd = dft4(x[0::2]), dft4(x[1::2])
    odd = [rotate(v, 4 * k) for k, v in enumerate(odd)]
    return [add(a, b) for a, b in zip(even, odd)] + [sub(a, b) for a, b in zip(even, odd)]


def dft32(load, store):
    parts = []
    for r in range(4):
        part = dft8([load(4 * i + r) for i in range(8)])
        parts.append([rotate(v, r * k) for k, v in enumerate(part)])
    for k in range(8):
        for q, value in enumerate(dft4([parts[r][k] for r in range(4)])):
            store(k + 8 * q, value)


def split(value):
    high = value.astype(jnp.bfloat16)
    return high, (value - high.astype(jnp.float32)).astype(jnp.bfloat16)


def matmul3(high_ref, low_ref, mat_ref, out_ref):
    dot = functools.partial(jnp.dot, preferred_element_type=jnp.float32)
    high, low = high_ref[...], low_ref[...]
    out_ref[...] = dot(high, mat_ref[0]) + dot(low, mat_ref[0]) + dot(high, mat_ref[1])


def tile(i):
    return pl.ds(i * LANES, LANES)


def short_stage(planes, row0, col_ref, tw_ref, z_ref, z_row):
    def load(a):
        w = col_ref[:, tile(a)]
        return tuple(p[pl.ds(row0, SUB), tile(a)] * w for p in planes)

    def store(k, value):
        real, imag = value
        if k:
            c, s = tw_ref[0, pl.ds(k * SUB, SUB), :], tw_ref[1, pl.ds(k * SUB, SUB), :]
            real, imag = real * c - imag * s, real * s + imag * c
        z_ref[0, pl.ds(z_row + k * SUB, SUB), :] = real
        z_ref[1, pl.ds(z_row + k * SUB, SUB), :] = imag

    dft32(load, store)


def matrix_kernel(target_ref, source_ref, base_ref, forward_ref, backward_ref):
    dot = functools.partial(jnp.dot, preferred_element_type=jnp.float32)
    square = (LONG, LONG)
    for frame in range(len(ORDERS)):
        wanted = jnp.broadcast_to(target_ref[pl.ds(frame, 1), :], square)
        pick = (wanted == lax.broadcasted_iota(jnp.int32, square, 0)).astype(jnp.bfloat16)
        wanted = jnp.broadcast_to(source_ref[:, pl.ds(frame, 1)], square)
        place = (wanted == lax.broadcasted_iota(jnp.int32, square, 1)).astype(jnp.bfloat16)
        for part in range(2):
            for half in range(2):
                forward_ref[frame, part, :, tile(half)] = dot(base_ref[part, :, tile(half)], pick).astype(jnp.bfloat16)
                backward_ref[frame, part, tile(half), :] = dot(place, base_ref[part, tile(half), :]).astype(jnp.bfloat16)


def last_kernel(real_ref, imag_ref, out_a_ref, out_b_ref, rows_ref, sem):
    copies = [
        pltpu.make_async_copy(ref.at[:, pl.ds(SHORT - SUB, SUB)], rows_ref.at[plane], sem.at[plane])
        for plane, ref in enumerate((real_ref, imag_ref))
    ]
    for copy in copies:
        copy.start()
    for plane, copy in enumerate(copies):
        copy.wait()
        for frame in range(FRAMES):
            out = (out_a_ref, out_b_ref)[frame // 4]
            out[plane, pl.ds(frame % 4 * 2, 2), :] = rows_ref[plane, frame, pl.ds(SUB - 2, 2), :]


def short_kernel(real_ref, imag_ref, col_ref, tw_ref, target_ref, source_ref, base_ref, *refs):
    zs, (forward_ref, backward_ref, x_ref, sem) = refs[:-4], refs[-4:]

    def fetch(frame, plane):
        return pltpu.make_async_copy((real_ref, imag_ref)[plane].at[frame], x_ref.at[frame, plane], sem.at[frame, plane])

    for frame in range(FRAMES):
        for plane in range(2):
            fetch(frame, plane).start()

    matrix_kernel(target_ref, source_ref, base_ref, forward_ref, backward_ref)

    for (first, count), z_ref in zip(GROUPS, zs):

        @pl.loop(0, count)
        def _(local):
            frame = first + local
            for plane in range(2):
                fetch(frame, plane).wait()
            planes, z = (x_ref.at[frame, 0], x_ref.at[frame, 1]), z_ref.at[local]

            @pl.loop(0, 4)
            def _(block):
                row = pl.multiple_of(block * SUB, SUB)
                short_stage(planes, row, col_ref, tw_ref, z, pl.multiple_of(row * SHORT, SUB * SHORT))


def edge_kernel(halo_ref, col_ref, tw_ref, out_ref):
    short_stage((halo_ref.at[0], halo_ref.at[1]), 0, col_ref, tw_ref, out_ref, 0)


def pre_kernel(row_ref, z_ref, edge_ref, mat_ref, keep_ref, send_ref, high_ref, low_ref, y_ref, *, first):
    local = pl.program_id(0)
    frame = first + local
    for plane in range(2):

        def rows(js):
            return z_ref[local, plane, pl.ds(js, LANES, stride=SUB), :]

        def rows_before(js):
            edge = edge_ref[plane, pl.ds(frame % 4 * 2 + js - 6, SHORT, stride=SUB), :]
            return jnp.concatenate([edge, z_ref[local, plane, pl.ds(js, 3 * SHORT, stride=SUB), :]], axis=0)

        before = rows_before(7)
        slope = before - rows_before(6)
        for js in range(SUB):
            now = rows(js)
            new_slope = now - before
            value = new_slope - slope
            before, slope = now, new_slope
            for b in range(4):
                part = value[b * SHORT : (b + 1) * SHORT].reshape(SHORT // SUB, SUB, LANES)
                part = part * row_ref[pl.ds((b * SUB + js) * SUB, SUB), :]
                high, low = split(part.reshape(SHORT, LANES))
                high_ref[pl.ds(js * LANES + b * SHORT, SHORT), tile(plane)] = high
                low_ref[pl.ds(js * LANES + b * SHORT, SHORT), tile(plane)] = low

    matmul3(high_ref, low_ref, mat_ref.at[frame], y_ref)

    for plane in range(2):
        outs = [ref.at[local, plane].reshape(SLOTS * SUB, LANES) for ref in (keep_ref, send_ref)]
        for js in range(SUB):
            piece = y_ref[pl.ds(js * LANES, LANES), tile(plane)].T
            for half, flat in enumerate(outs):
                flat[pl.ds(js, SLOTS, stride=SUB), :] = piece[half * SLOTS : (half + 1) * SLOTS]


def gather_kernel(first_ref, second_ref, keep_ref, send_ref, *, step):
    left = SLOTS // 2 >> step

    @pl.loop(0, SLOTS // 2, step=SUB)
    def _(at):
        base = 2 * at - at % left if left >= SUB else 2 * at
        for half, ref in enumerate((first_ref, second_ref)):
            for plane in range(2):
                for slot in range(SUB):
                    source = base + (slot if left >= SUB else 2 * slot - slot % left)
                    for side, out in enumerate((keep_ref, send_ref)):
                        out[plane, half * (SLOTS // 2) + at + slot] = ref[plane, source + side * left]


def copies_out(wide_ref, outs, sem, frame):
    return [pltpu.make_async_copy(wide_ref.at[plane], outs[plane].at[frame], sem.at[plane]) for plane in range(2)]


def post_kernel(keep_ref, got_ref, tw_ref, mat_ref, *refs, frame):
    wide_ref, sem, high_ref, low_ref, y_ref = refs[-5:]
    if frame:
        copies = copies_out(refs[0], refs[-7:-5], sem, frame - 1)
        for copy in copies:
            copy.start()
    for plane in range(2):
        flats = [ref.at[plane].reshape(SLOTS * SUB, LANES) for ref in (keep_ref, got_ref)]
        for js in range(SUB):
            pieces = [flat[pl.ds(js, SLOTS, stride=SUB), :] for flat in flats]
            high, low = split(jnp.concatenate(pieces, axis=0).T)
            high_ref[pl.ds(js * LANES, LANES), tile(plane)] = high
            low_ref[pl.ds(js * LANES, LANES), tile(plane)] = low

    matmul3(high_ref, low_ref, mat_ref.at[frame], y_ref)

    @pl.loop(0, 4)
    def _(block):
        at = pl.multiple_of(block * SUB, SUB)

        def load(j):
            row = pl.ds(((j % SUB) * 4 + j // SUB) * SHORT + at, SUB)
            real, imag = y_ref[row, tile(0)], y_ref[row, tile(1)]
            if j:
                c, s = tw_ref[0, pl.ds(j * SUB, SUB), :], tw_ref[1, pl.ds(j * SUB, SUB), :]
                real, imag = real * c - imag * s, real * s + imag * c
            return real, imag

        def store(k, value):
            for plane in range(2):
                wide_ref[plane, pl.ds(at, SUB), tile(k)] = value[plane]

        dft32(load, store)

    if frame:
        for copy in copies:
            copy.wait()


def flush_kernel(wide_ref, *refs):
    for copy in copies_out(wide_ref, refs[-3:-1], refs[-1], FRAMES - 1):
        copy.start()
    for copy in copies_out(wide_ref, refs[-3:-1], refs[-1], FRAMES - 1):
        copy.wait()


VMEM = pl.BlockSpec(memory_space=pltpu.VMEM)
ANY = pl.BlockSpec(memory_space=pl.ANY)
PARAMS = pltpu.CompilerParams(vmem_limit_bytes=12 * 2**20)


def cost(flops):
    return pl.CostEstimate(flops=flops, bytes_accessed=2**21, transcendentals=0)


def in_hbm(*arrays):
    return [pltpu.with_memory_space_constraint(x, pltpu.HBM) for x in arrays]


def last_rows(real, imag):
    half = jax.ShapeDtypeStruct((2, SUB, N), jnp.float32)
    return pl.pallas_call(
        last_kernel,
        in_specs=[ANY] * 2,
        out_specs=[VMEM] * 2,
        out_shape=[half] * 2,
        scratch_shapes=[pltpu.VMEM((2, FRAMES, SUB, N), jnp.float32), pltpu.SemaphoreType.DMA((2,))],
        compiler_params=PARAMS,
        cost_estimate=cost(10**6),
        name="last",
    )(*in_hbm(real, imag))


def short(real, imag, col, tw, target, source):
    matrix = jax.ShapeDtypeStruct((FRAMES, 2, 2 * LONG, 2 * LONG), jnp.bfloat16)
    *zs, forward, backward = pl.pallas_call(
        short_kernel,
        in_specs=[ANY] * 2 + [VMEM] * 5,
        out_specs=[VMEM] * (len(GROUPS) + 2),
        out_shape=[jax.ShapeDtypeStruct((count, 2, ROWS, LANES), jnp.float32) for _, count in GROUPS] + [matrix] * 2,
        scratch_shapes=[pltpu.VMEM((FRAMES, 2, SHORT, N), jnp.float32), pltpu.SemaphoreType.DMA((FRAMES, 2))],
        compiler_params=PARAMS,
        cost_estimate=cost(10**9),
        name="short",
    )(*in_hbm(real, imag), col, tw, target, source, jnp.asarray(long_matrix()))
    return zs, forward, backward


def edges(halo, col, tw):
    return pl.pallas_call(
        edge_kernel,
        in_specs=[VMEM] * 3,
        out_specs=VMEM,
        out_shape=jax.ShapeDtypeStruct((2, SHORT * SUB, LANES), jnp.float32),
        compiler_params=PARAMS,
        cost_estimate=cost(10**6),
        name="edges",
    )(halo, col, tw)


def pre(first, count, row, z, edge, mat):
    f32 = jnp.float32
    half = jax.ShapeDtypeStruct((count, 2, SLOTS, SUB, LANES), f32)
    return pl.pallas_call(
        functools.partial(pre_kernel, first=first),
        grid=(count,),
        in_specs=[VMEM] * 4,
        out_specs=[VMEM, VMEM],
        out_shape=[half, half],
        scratch_shapes=[
            pltpu.VMEM((ROWS, 2 * LANES), jnp.bfloat16),
            pltpu.VMEM((ROWS, 2 * LANES), jnp.bfloat16),
            pltpu.VMEM((ROWS, 2 * LANES), f32),
        ],
        compiler_params=PARAMS,
        cost_estimate=cost(5 * 10**8 * count),
    )(row, z, edge, mat)


WIDE = jax.ShapeDtypeStruct((2, SHORT, N), jnp.float32)
OUT = jax.ShapeDtypeStruct((FRAMES, SHORT, N), jnp.float32)


def post(frame, keep, got, tw, mat, before, outs):
    out_shape, out_specs = ([OUT] * 2, [ANY] * 2) if frame else ([], [])
    results = pl.pallas_call(
        functools.partial(post_kernel, frame=frame),
        in_specs=[VMEM] * (5 if frame else 4) + [ANY] * len(outs),
        out_specs=out_specs + [VMEM],
        out_shape=out_shape + [WIDE],
        input_output_aliases={5 + i: i for i in range(len(outs))},
        scratch_shapes=[
            pltpu.SemaphoreType.DMA((2,)),
            pltpu.VMEM((ROWS, 2 * LANES), jnp.bfloat16),
            pltpu.VMEM((ROWS, 2 * LANES), jnp.bfloat16),
            pltpu.VMEM((ROWS, 2 * LANES), jnp.float32),
        ],
        compiler_params=PARAMS,
        cost_estimate=cost(10**9),
    )(keep, got, tw, mat, *([before] if frame else []), *outs)
    return results[-1], tuple(results[:-1])


def flush(wide, outs):
    return pl.pallas_call(
        flush_kernel,
        in_specs=[VMEM] + [ANY] * 2,
        out_specs=[ANY] * 2,
        out_shape=[OUT] * 2,
        input_output_aliases={1: 0, 2: 1},
        scratch_shapes=[pltpu.SemaphoreType.DMA((2,))],
        compiler_params=PARAMS,
        cost_estimate=cost(10**6),
        name="flush",
    )(wide, *outs)


def gather(step, first, second):
    half = jax.ShapeDtypeStruct((2, SLOTS, SUB, LANES), jnp.float32)
    (one, at_one), (two, at_two) = first, second

    def kernel(one_ref, two_ref, keep_ref, send_ref):
        gather_kernel(one_ref.at[at_one], two_ref.at[at_two], keep_ref, send_ref, step=step)

    return pl.pallas_call(
        kernel,
        in_specs=[VMEM] * 2,
        out_specs=[VMEM] * 2,
        out_shape=[half] * 2,
        compiler_params=pltpu.CompilerParams(vmem_limit_bytes=2**20),
        cost_estimate=cost(10**5),
        name="gather",
    )(one, two)


def permute(value, pairs):
    return lax.ppermute(value, "pa", pairs)


def exchange(frame, halves):
    for step in range(STEPS):
        keep, send = gather(step, *halves)
        got = permute(send, edge_pairs(frame, step))
        halves = (keep[None], 0), (got[None], 0)
    if frame in LATE:
        keep, send = gather(STEPS - 1, *halves)
        got = permute(send, CORES)
    return keep, got


def on_device(real, imag):
    frames, rows, _ = real.shape
    me = lax.axis_index("pa")
    halos = [permute(last, [(d, d + 1) for d in range(2 * SLOTS - 1)]) for last in last_rows(real, imag)]
    row = hamming(me * rows + jnp.arange(rows, dtype=jnp.int32)) * (1.0 / (math.sqrt(6.0) * N))
    row = jnp.broadcast_to(row[:, None, None], (rows, SUB, LANES)).reshape(rows * SUB, LANES)
    col = jnp.asarray(column_window())
    tw = jnp.asarray(twiddles())
    target, source = devices(me, True), devices(me, False)
    z, forward, backward = short(real, imag, col, tw, target, source)
    edge = [edges(halo, col, tw) for halo in halos]
    halves = []
    for (first, count), part in zip(GROUPS, z):
        keep, send = pre(first, count, row, part, edge[first // 4], forward)
        if first not in LATE:
            send = permute(send, CORES)
        halves += [((keep, i), (send, i)) for i in range(count)]
    ends = [exchange(frame, halves[frame]) for frame in range(frames)]
    wide, outs = None, ()
    for frame in range(frames):
        wide, outs = post(frame, *ends[frame], tw, backward, wide, outs)
    return tuple(flush(wide, outs))


def solution(mesh):
    placed = (P(None, "pa", None), P(None, "pa", None))
    return jax.shard_map(on_device, mesh=mesh, in_specs=placed, out_specs=placed, check_vma=False)
```
